128 devices in a mesh: rep: 1, data: 2 (over core), model: 64 (over z, y, x).
Axes of the slice: x: 4, y: 4, z: 4, core: 2. Of those that a mesh axis runs over, the one named last changes fastest.
Arguments:
- x: bfloat16 [4, 2048, 1024], P(('rep', 'data'), 'model')
- lengths: int32 [4], P(('rep', 'data'))
- gamma: bfloat16 [2, 1024], P(None, 'data')
- w_in: bfloat16 [2, 1024, 147456], P(None, 'data', 'model')
- w_kv: bfloat16 [2, 1024, 256], P(None, 'data')
- w_out: bfloat16 [2, 81920, 1024], P(None, 'model', 'data')
Outputs:
- output: bfloat16 [4, 2048, 1024], P(('rep', 'data'), 'model')
All inputs are finite; a program needn't handle non-finite values.
Results may differ from the reference program's by a relative error of at most 0.02.
Values are sent between devices in bfloat16 or wider.
A program may use at most 1 GiB of HBM per device.

```python
import jax
import jax.numpy as jnp
from jax import lax

BATCH_SIZE = 4
SEQ_LEN = 2048
D_MODEL = 1024
N_HEADS = 128
HEAD_DIM = 128
D_FF = 65536
N_SHARDS = 64

EPSILON = 1e-6
LOCAL_HEADS = N_HEADS // N_SHARDS
FF_LOCAL = D_FF // N_SHARDS
ATTN_COLS = LOCAL_HEADS * HEAD_DIM
IN_LOCAL = ATTN_COLS + 2 * FF_LOCAL
OUT_LOCAL = ATTN_COLS + FF_LOCAL
QUERY_BLOCK = SEQ_LEN // N_SHARDS


def setup_inputs(seed: int = 0, part: int = 0) -> dict:
    part_key = jax.random.fold_in(jax.random.key(seed), part)
    key_x, key_len_a, key_len_b = jax.random.split(part_key, 3)
    key_gain, key_in, key_kv, key_out = jax.random.split(jax.random.key(seed + 1), 4)
    x = jax.random.normal(key_x, (BATCH_SIZE, SEQ_LEN, D_MODEL), jnp.float32).astype(jnp.bfloat16)
    len_min = SEQ_LEN // 8
    len_a = jax.random.randint(key_len_a, (BATCH_SIZE,), len_min, SEQ_LEN + 1, jnp.int32)
    len_b = jax.random.randint(key_len_b, (BATCH_SIZE,), len_min, SEQ_LEN + 1, jnp.int32)
    lengths = jnp.maximum(len_a, len_b).at[0].set(SEQ_LEN).at[BATCH_SIZE - 1].set(len_min)
    gamma = (1.0 + 0.3 * jax.random.normal(key_gain, (2, D_MODEL), jnp.float32)).astype(jnp.bfloat16)
    w_in = (jax.random.normal(key_in, (2, D_MODEL, N_SHARDS * IN_LOCAL), jnp.float32) * D_MODEL ** -0.5).astype(jnp.bfloat16)
    w_kv = (jax.random.normal(key_kv, (2, D_MODEL, 2 * HEAD_DIM), jnp.float32) * (2.0 * D_MODEL ** -0.5)).astype(jnp.bfloat16)
    w_out = (jax.random.normal(key_out, (2, N_SHARDS * OUT_LOCAL, D_MODEL), jnp.float32) * (N_SHARDS * OUT_LOCAL) ** -0.5).astype(jnp.bfloat16)
    return {"x": x, "lengths": lengths, "gamma": gamma, "w_in": w_in, "w_kv": w_kv, "w_out": w_out}


def rms_norm(x_in, gain):
    x_f32 = x_in.astype(jnp.float32)
    inv_rms = lax.rsqrt(jnp.mean(x_f32 * x_f32, axis=-1, keepdims=True) + EPSILON)
    return (x_f32 * inv_rms * gain.astype(jnp.float32)).astype(jnp.bfloat16)


def attend_one(q_seq, k_seq, v_seq, seq_len):
    key_pos = jnp.arange(SEQ_LEN)
    q_blocks = q_seq.reshape(N_SHARDS, QUERY_BLOCK, N_HEADS, HEAD_DIM)
    k_f32 = k_seq.astype(jnp.float32)
    v_f32 = v_seq.astype(jnp.float32)

    def one_block(block_in):
        q_blk, blk_idx = block_in
        scores = jnp.einsum("qhd,kd->hqk", q_blk.astype(jnp.float32), k_f32) * (HEAD_DIM ** -0.5)
        q_pos = blk_idx * QUERY_BLOCK + jnp.arange(QUERY_BLOCK)
        visible = (key_pos[None, :] <= q_pos[:, None]) & (key_pos[None, :] < seq_len)
        scores = jnp.where(visible[None], scores, -1e30)
        attn_probs = jax.nn.softmax(scores, axis=-1).astype(jnp.bfloat16)
        blk_out = jnp.einsum("hqk,kd->qhd", attn_probs.astype(jnp.float32), v_f32)
        return blk_out.astype(jnp.bfloat16)

    blocks_out = lax.map(one_block, (q_blocks, jnp.arange(N_SHARDS)))
    return blocks_out.reshape(SEQ_LEN, N_SHARDS, ATTN_COLS)


def layer_one(x_seq, seq_len, gain, w_in_l, w_kv_l, w_out_l):
    normed = rms_norm(x_seq, gain)
    projected = jnp.dot(normed, w_in_l, preferred_element_type=jnp.float32).astype(jnp.bfloat16)
    projected = projected.reshape(SEQ_LEN, N_SHARDS, IN_LOCAL)
    queries = projected[:, :, :ATTN_COLS].reshape(SEQ_LEN, N_HEADS, HEAD_DIM)
    gate = projected[:, :, ATTN_COLS:ATTN_COLS + FF_LOCAL].astype(jnp.float32)
    up_proj = projected[:, :, ATTN_COLS + FF_LOCAL:].astype(jnp.float32)
    key_value = jnp.dot(normed, w_kv_l, preferred_element_type=jnp.float32).astype(jnp.bfloat16)
    attn_out = attend_one(queries, key_value[:, :HEAD_DIM], key_value[:, HEAD_DIM:], seq_len)
    mlp_out = (jax.nn.silu(gate) * up_proj).astype(jnp.bfloat16)
    mixed = jnp.moveaxis(jnp.concatenate([attn_out, mlp_out], axis=-1), 1, 0)
    w_out_groups = w_out_l.reshape(N_SHARDS, OUT_LOCAL, D_MODEL)

    def add_group(z_acc, group_in):
        rows, weights = group_in
        part_z = jnp.dot(rows, weights, preferred_element_type=jnp.float32).astype(jnp.bfloat16)
        return z_acc + part_z.astype(jnp.float32), None

    z_sum, _ = lax.scan(add_group, jnp.zeros((SEQ_LEN, D_MODEL), jnp.float32), (mixed, w_out_groups))
    return (x_seq.astype(jnp.float32) + z_sum).astype(jnp.bfloat16)


def reference(x, lengths, gamma, w_in, w_kv, w_out):
    def one_layer(hidden, params):
        gain, w_in_l, w_kv_l, w_out_l = params
        new_hidden = lax.map(lambda seq_in: layer_one(seq_in[0], seq_in[1], gain, w_in_l, w_kv_l, w_out_l), (hidden, lengths))
        return new_hidden, None

    result, _ = lax.scan(one_layer, x, (gamma, w_in, w_kv, w_out))
    return result
```

```python
import functools

import jax
import jax.numpy as jnp
from jax import lax
from jax.experimental import pallas as pl
from jax.experimental.pallas import tpu as pltpu
from jax.sharding import PartitionSpec as P

EPSILON = 1e-6
MESH = pl.DeviceIdType.MESH
F32 = jnp.float32
BF16 = jnp.bfloat16

SIDE = 4
ROWS = 32
D_MODEL = 1024
HEAD = 128
ATTN = 256
FF = 1024
TILE = SIDE * SIDE * ROWS
N_TILES = SIDE
STRIDE = (16, 4, 1)
COLS = ((0, 384), (384, 384), (768, 256))
AG_ORDER = ((2, 1, 0), (1, 0, 2), (0, 2, 1))
RS_ORDER = tuple(tuple(reversed(order)) for order in AG_ORDER)
POINTS = 6
NEG = -1e30


def kernel(
    x_ref, len_ref, gamma_ref, w_in_ref, w_kv_ref, w_out_ref, y_ref,
    win, wkv, wout, gfull, hbuf, zbuf, xcur,
    ra0, ra1, ra2, rb0, rb1, rb2,
    k_t, v_ext, q_ext, acc, row_max, mixed,
    ag_send, ag_recv, rs_send, rs_recv, w_local, w_send, w_recv, g_local, g_send, g_recv,
):
    m = lax.axis_index("model")
    core = lax.axis_index("data")
    other = 1 - core
    pos = (lax.div(m, 16), lax.rem(lax.div(m, 4), 4), lax.rem(m, 4))
    ra = (ra0, ra1, ra2)
    rb = (rb0, rb1, rb2)

    def shift(axis, delta):
        return lax.rem(pos[axis] + delta + SIDE, SIDE)

    def neighbour(axis, delta):
        return {"model": m + (shift(axis, delta) - pos[axis]) * STRIDE[axis]}

    barrier = pltpu.get_barrier_semaphore()
    for axis in range(3):
        for delta in (1, -1):
            pl.semaphore_signal(barrier, inc=1, device_id=neighbour(axis, delta), device_id_type=MESH)
    pl.semaphore_signal(barrier, inc=1, device_id={"data": other}, device_id_type=MESH)
    pl.semaphore_wait(barrier, 7)

    pairs = ((w_in_ref, win), (w_kv_ref, wkv), (w_out_ref, wout))

    def weight_local(layer, i):
        src, dst = pairs[i]
        return pltpu.make_async_copy(src.at[layer], dst.at[layer, core], w_local.at[layer, i])

    def weight_send(layer, i):
        src, dst = pairs[i]
        return pltpu.make_async_remote_copy(
            src_ref=src.at[layer], dst_ref=dst.at[layer, core], send_sem=w_send.at[layer, i],
            recv_sem=w_recv.at[layer, i], device_id={"data": other}, device_id_type=MESH)

    def weight_arrival(layer, i):
        src, dst = pairs[i]
        return pltpu.make_async_remote_copy(
            src_ref=src.at[layer], dst_ref=dst.at[layer, other], send_sem=w_send.at[layer, i],
            recv_sem=w_recv.at[layer, i], device_id={"data": other}, device_id_type=MESH)

    def weights_start(layer):
        for i in range(3):
            weight_send(layer, i).start()
            weight_local(layer, i).start()

    def weights_wait(layer):
        for i in range(3):
            weight_local(layer, i).wait()
            weight_send(layer, i).wait_send()
            weight_arrival(layer, i).wait_recv()

    gain_local = pltpu.make_async_copy(gamma_ref, gfull.at[core], g_local)
    gain_send = pltpu.make_async_remote_copy(
        src_ref=gamma_ref, dst_ref=gfull.at[core], send_sem=g_send, recv_sem=g_recv,
        device_id={"data": other}, device_id_type=MESH)
    gain_arrival = pltpu.make_async_remote_copy(
        src_ref=gamma_ref, dst_ref=gfull.at[other], send_sem=g_send, recv_sem=g_recv,
        device_id={"data": other}, device_id_type=MESH)
    gain_send.start()
    gain_local.start()
    weights_start(0)

    def h_block(b, part, phase, index, rows):
        order = AG_ORDER[part]
        where = [slice(None)] * 3
        for axis in order[phase + 1:]:
            where[axis] = pos[axis]
        where[order[phase]] = index
        lo, width = COLS[part]
        return hbuf.at[(b, *where, pl.ds(*rows), pl.ds(lo, width))]

    HALVES = ((0, ROWS // 2), (ROWS // 2, ROWS // 2))
    WHOLE = (0, ROWS)

    def ag_copy(b, part, phase, slot, index, rows, delta):
        block = h_block(b, part, phase, index, rows)
        return pltpu.make_async_remote_copy(
            src_ref=block, dst_ref=block, send_sem=ag_send.at[b, part, phase, slot],
            recv_sem=ag_recv.at[b, part, phase, slot],
            device_id=neighbour(AG_ORDER[part][phase], delta), device_id_type=MESH)

    def ag_sent(b, part, phase, slot):
        axis = AG_ORDER[part][phase]
        if slot == 0:
            return ag_copy(b, part, phase, 0, pos[axis], WHOLE, 1)
        if slot == 1:
            return ag_copy(b, part, phase, 1, pos[axis], WHOLE, -1)
        if slot == 2:
            return ag_copy(b, part, phase, 2, shift(axis, -1), HALVES[0], 1)
        return ag_copy(b, part, phase, 3, shift(axis, 1), HALVES[1], -1)

    def ag_arrival(b, part, phase, slot):
        axis = AG_ORDER[part][phase]
        if slot == 0:
            return ag_copy(b, part, phase, 0, shift(axis, -1), WHOLE, 1)
        if slot == 1:
            return ag_copy(b, part, phase, 1, shift(axis, 1), WHOLE, -1)
        if slot == 2:
            return ag_copy(b, part, phase, 2, shift(axis, 2), HALVES[0], 1)
        return ag_copy(b, part, phase, 3, shift(axis, 2), HALVES[1], -1)

    def ag_step(b, stage):
        phase, second = stage // 2, stage % 2
        for part in range(3):
            if stage:
                before, was_second = (stage - 1) // 2, (stage - 1) % 2
                for slot in ((2, 3) if was_second else (0, 1)):
                    ag_arrival(b, part, before, slot).wait_recv()
            if stage < 6:
                for slot in ((2, 3) if second else (0, 1)):
                    ag_sent(b, part, phase, slot).start()
        if stage == 6:
            for part in range(3):
                for k in range(3):
                    for slot in range(4):
                        ag_sent(b, part, k, slot).wait_send()

    def z_where(b, part, phase, index):
        order = RS_ORDER[part]
        where = [None] * 3
        for axis in order[:phase]:
            where[axis] = pos[axis]
        where[order[phase]] = index
        return where

    def z_block(b, part, phase, index, rows):
        where = [slice(None) if i is None else i for i in z_where(b, part, phase, index)]
        lo, width = COLS[part]
        return zbuf.at[(b, *where, pl.ds(*rows), pl.ds(lo, width))]

    def r_block(buf, b, part, phase, side, rows):
        lo, width = COLS[part]
        return buf[phase].at[(b, side, *([slice(None)] * (2 - phase)), pl.ds(*rows), pl.ds(lo, width))]

    def rs_copy(b, part, phase, slot):
        axis = RS_ORDER[part][phase]
        if slot == 0:
            src = z_block(b, part, phase, shift(axis, 2), HALVES[0])
            dst, delta = r_block(ra, b, part, phase, 0, (0, ROWS // 2)), -1
        elif slot == 1:
            src = z_block(b, part, phase, shift(axis, 2), HALVES[1])
            dst, delta = r_block(ra, b, part, phase, 1, (0, ROWS // 2)), 1
        elif slot == 2:
            src = z_block(b, part, phase, shift(axis, -1), WHOLE)
            dst, delta = r_block(rb, b, part, phase, 0, WHOLE), -1
        else:
            src = z_block(b, part, phase, shift(axis, 1), WHOLE)
            dst, delta = r_block(rb, b, part, phase, 1, WHOLE), 1
        return pltpu.make_async_remote_copy(
            src_ref=src, dst_ref=dst, send_sem=rs_send.at[b, part, phase, slot],
            recv_sem=rs_recv.at[b, part, phase, slot],
            device_id=neighbour(axis, delta), device_id_type=MESH)

    def add_into(b, part, phase, index, rows, sources):
        where = z_where(b, part, phase, index)
        free = [i for i in range(3) if where[i] is None]
        lo, width = COLS[part]

        def one(i):
            at = list(where)
            lead = ()
            if free:
                at[free[0]] = i
                lead = (i,)
            at = [slice(None) if j is None else j for j in at]
            target = (b, *at, pl.ds(*rows), pl.ds(lo, width))
            total = zbuf[target].astype(F32)
            for buf, side in sources:
                rest = [slice(None)] * (len(free) - len(lead))
                height = rows[1]
                total = total + buf[phase][(b, side, *lead, *rest, pl.ds(0, height), pl.ds(lo, width))].astype(F32)
            zbuf[target] = total.astype(BF16)

        if len(free) == 2:
            @pl.loop(0, SIDE)
            def _(i):
                one(i)
        elif len(free) == 1:
            for i in range(SIDE):
                one(i)
        else:
            one(None)

    def rs_step(b, stage):
        phase, second = stage // 2, stage % 2
        for part in range(3):
            if stage:
                before, was_second = (stage - 1) // 2, (stage - 1) % 2
                axis = RS_ORDER[part][before]
                for slot in ((2, 3) if was_second else (0, 1)):
                    rs_copy(b, part, before, slot).wait_recv()
                if was_second:
                    add_into(b, part, before, pos[axis], WHOLE, ((rb, 0), (rb, 1)))
                else:
                    add_into(b, part, before, shift(axis, -1), HALVES[0], ((ra, 0),))
                    add_into(b, part, before, shift(axis, 1), HALVES[1], ((ra, 1),))
            if stage < 6:
                for slot in ((2, 3) if second else (0, 1)):
                    rs_copy(b, part, phase, slot).start()
        if stage == 6:
            for part in range(3):
                for k in range(3):
                    for slot in range(4):
                        rs_copy(b, part, k, slot).wait_send()

    def norm(b, layer):
        x = xcur[b].astype(F32)
        gain = jnp.concatenate([gfull[0, layer:layer + 1, :], gfull[1, layer:layer + 1, :]], axis=1).astype(F32)
        inv = lax.rsqrt(jnp.mean(x * x, axis=-1, keepdims=True) + EPSILON)
        hbuf[b, pos[0], pos[1], pos[2]] = (x * inv * gain).astype(BF16)

    def residual(b):
        z = zbuf[b, pos[0], pos[1], pos[2]].astype(F32)
        xcur[b] = (xcur[b].astype(F32) + z).astype(BF16)

    xcur[...] = x_ref[...]
    gain_local.wait()
    gain_send.wait_send()
    gain_arrival.wait_recv()
    norm(0, 0)
    ag_step(0, 0)
    norm(1, 0)
    rows_i = lax.broadcasted_iota(jnp.int32, (HEAD, TILE), 0)
    q_ext[:, HEAD:] = jnp.where(lax.broadcasted_iota(jnp.int32, (2 * TILE, HEAD), 1) == 0, 1.0, 0.0).astype(BF16)
    v_ext[:, :, HEAD:] = jnp.ones((N_TILES, TILE, HEAD), BF16)
    for stage in range(1, 6):
        ag_step(0, stage)
    ag_step(1, 0)
    ag_step(0, 6)
    weights_wait(0)
    weights_start(1)

    plan = {}

    def at(seg, tick, kind, b, stage):
        plan.setdefault(divmod(seg * N_TILES * POINTS + tick, POINTS), []).append((kind, b, stage))

    for stage, tick in zip(range(1, 7), (2, 4, 7, 9, 17, 22)):
        at(0, tick, "ag", 1, stage)
    for stage, tick in zip(range(0, 7), (0, 4, 10, 12, 14, 16, 18)):
        at(1, tick, "rs", 0, stage)
    at(1, 18, "turn", 0, 0)
    for stage, tick in zip(range(0, 3), (18, 20, 22)):
        at(1, tick, "ag", 0, stage)
    at(2, 0, "rs", 1, 0)
    for stage in range(3, 7):
        at(2, 0, "ag", 0, stage)
    at(2, 0, "weights", 0, 1)
    for stage, tick in zip(range(1, 7), (1, 6, 8, 10, 12, 14)):
        at(2, tick, "rs", 1, stage)
    at(2, 14, "turn", 1, 0)
    for stage, tick in zip(range(0, 5), (14, 16, 18, 21, 23)):
        at(2, tick, "ag", 1, stage)
    at(3, 0, "rs", 0, 0)
    for stage in range(5, 7):
        at(3, 0, "ag", 1, stage)
    for stage, tick in zip(range(1, 7), (4, 11, 13, 15, 17, 19)):
        at(3, tick, "rs", 0, stage)

    def run(kind, b, stage):
        if kind == "ag":
            ag_step(b, stage)
        elif kind == "rs":
            rs_step(b, stage)
        elif kind == "weights":
            weights_wait(stage)
        else:
            residual(b)
            norm(b, 1)

    scale = float(HEAD ** -0.5 * 1.4426950408889634)
    CHUNK = 256

    def attend(j, diag):
        for lo in range(0, 2 * TILE, CHUNK):
            rows = pl.ds(lo, CHUNK)
            s = jnp.dot(q_ext[rows, :], k_t[j], preferred_element_type=F32)
            if diag:
                q_pos = (lo % TILE) + lax.broadcasted_iota(jnp.int32, (CHUNK, TILE), 0)
                s = jnp.where(lax.broadcasted_iota(jnp.int32, (CHUNK, TILE), 1) <= q_pos, s, NEG)
            top = jnp.max(s, axis=-1, keepdims=True)
            if diag:
                new = top
            else:
                old = row_max[rows, :1]
                new = jnp.maximum(old, top)
            p = jnp.exp2((s - new) * scale).astype(BF16)
            out = jnp.dot(p, v_ext[j], preferred_element_type=F32)
            if diag:
                acc[rows, :] = out
            else:
                acc[rows, :] = acc[rows, :] * jnp.exp2((old - new) * scale) + out
            row_max[rows, :] = jnp.broadcast_to(new, (CHUNK, HEAD))

    @pl.loop(0, 4 * N_TILES)
    def _(it):
        seg, t = lax.div(it, N_TILES), lax.rem(it, N_TILES)
        layer, b = lax.div(seg, 2), lax.rem(seg, 2)

        def tick(point):
            for (when, where), steps in plan.items():
                if where == point:
                    @pl.when(it == when)
                    def _(steps=steps):
                        for step in steps:
                            run(*step)

        tick(0)
        h = hbuf[b, t].reshape(TILE, D_MODEL)
        kv = jnp.dot(h, wkv[layer].reshape(D_MODEL, 2 * HEAD), preferred_element_type=F32).astype(BF16)
        k_t[t, :HEAD, :] = kv[:, :HEAD].T
        key_pos = t * TILE + lax.broadcasted_iota(jnp.int32, (HEAD, TILE), 1)
        hidden = jnp.logical_and(rows_i == 0, key_pos >= len_ref[pl.ds(b, 1), :])
        k_t[t, HEAD:, :] = jnp.where(hidden, NEG, 0.0).astype(BF16)
        v_ext[t, :, :HEAD] = kv[:, HEAD:]
        q = jnp.dot(h, win[layer, :, :, :ATTN].reshape(D_MODEL, ATTN), preferred_element_type=F32).astype(BF16)
        q_ext[:TILE, :HEAD] = q[:, :HEAD]
        q_ext[TILE:, :HEAD] = q[:, HEAD:]
        tick(1)
        for i in range(2):
            h = hbuf[b, t].reshape(TILE, D_MODEL)
            lo = ATTN + i * 512
            g = jnp.dot(h, win[layer, :, :, lo:lo + 512].reshape(D_MODEL, 512), preferred_element_type=F32)
            u = jnp.dot(h, win[layer, :, :, lo + FF:lo + FF + 512].reshape(D_MODEL, 512), preferred_element_type=F32)
            g = g.astype(BF16).astype(F32)
            u = u.astype(BF16).astype(F32)
            mixed[:, lo:lo + 512] = (jax.nn.silu(g) * u).astype(BF16)
            tick(2 + i)
        attend(t, True)
        tick(4)

        @pl.loop(0, N_TILES - 1)
        def _(j):
            @pl.when(j < t)
            def _():
                attend(j, False)

        for head in range(2):
            rows = pl.ds(head * TILE, TILE)
            mixed[:, head * HEAD:(head + 1) * HEAD] = (acc[rows, :HEAD] / acc[rows, HEAD:]).astype(BF16)
        tick(5)
        for half in range(2):
            z = jnp.dot(mixed[...], wout[layer, half], preferred_element_type=F32).astype(BF16)
            zbuf[b, t, :, :, :, half * 512:(half + 1) * 512] = z.reshape(SIDE, SIDE, ROWS, 512)

    rs_step(1, 0)
    residual(0)
    y_ref[0] = xcur[0]
    for stage in range(1, 7):
        rs_step(1, stage)
    residual(1)
    y_ref[1] = xcur[1]


def local_step(x, lengths, gamma, w_in, w_kv, w_out):
    vmem = pl.BlockSpec(memory_space=pltpu.VMEM)
    hbm = pl.BlockSpec(memory_space=pl.ANY)
    dma = pltpu.SemaphoreType.DMA
    box = (SIDE, SIDE)
    scratch = [
        pltpu.VMEM((2, 2, 512, 2304), BF16),
        pltpu.VMEM((2, 2, 512, 256), BF16),
        pltpu.VMEM((2, 2, 1280, 512), BF16),
        pltpu.VMEM((2, 2, 512), BF16),
        pltpu.VMEM((2, SIDE, *box, ROWS, D_MODEL), BF16),
        pltpu.VMEM((2, SIDE, *box, ROWS, D_MODEL), BF16),
        pltpu.VMEM((2, ROWS, D_MODEL), BF16),
        pltpu.VMEM((2, 2, *box, ROWS // 2, D_MODEL), BF16),
        pltpu.VMEM((2, 2, SIDE, ROWS // 2, D_MODEL), BF16),
        pltpu.VMEM((2, 2, ROWS // 2, D_MODEL), BF16),
        pltpu.VMEM((2, 2, *box, ROWS, D_MODEL), BF16),
        pltpu.VMEM((2, 2, SIDE, ROWS, D_MODEL), BF16),
        pltpu.VMEM((2, 2, ROWS, D_MODEL), BF16),
        pltpu.VMEM((N_TILES, 2 * HEAD, TILE), BF16),
        pltpu.VMEM((N_TILES, TILE, 2 * HEAD), BF16),
        pltpu.VMEM((2 * TILE, 2 * HEAD), BF16),
        pltpu.VMEM((2 * TILE, 2 * HEAD), F32),
        pltpu.VMEM((2 * TILE, HEAD), F32),
        pltpu.VMEM((TILE, ATTN + FF), BF16),
        dma((2, 3, 3, 4)), dma((2, 3, 3, 4)), dma((2, 3, 3, 4)), dma((2, 3, 3, 4)),
        dma((2, 3)), dma((2, 3)), dma((2, 3)), dma, dma, dma,
    ]
    return pl.pallas_call(
        kernel,
        out_shape=jax.ShapeDtypeStruct(x.shape, x.dtype),
        in_specs=[vmem, vmem, vmem, hbm, hbm, hbm],
        out_specs=vmem,
        scratch_shapes=scratch,
        compiler_params=pltpu.CompilerParams(
            collective_id=0, has_side_effects=True, vmem_limit_bytes=67_043_328),
        name="layers",
    )(x, lengths.reshape(2, 1), gamma, w_in, w_kv, w_out)


def solution(mesh):
    batch_axes = ("rep", "data")
    in_specs = (
        P(batch_axes, "model", None),
        P(batch_axes),
        P(None, "data"),
        P(None, "data", "model"),
        P(None, "data", None),
        P(None, "model", "data"),
    )
    return jax.shard_map(local_step, mesh=mesh, in_specs=in_specs, out_specs=P(batch_axes, "model", None), check_vma=False)
```

```python
import functools

import jax
import jax.numpy as jnp
from jax import lax
from jax.experimental import pallas as pl
from jax.experimental.pallas import tpu as pltpu
from jax.sharding import PartitionSpec as P

EPSILON = 1e-6
MESH = pl.DeviceIdType.MESH
F32 = jnp.float32
BF16 = jnp.bfloat16

SIDE = 4
ROWS = 32
HALF = 16
D_MODEL = 1024
HEAD = 128
ATTN = 256
FF = 1024
TILE = SIDE * SIDE * HALF
N_TILES = SIDE
STRIDE = (16, 4, 1)
WIDTHS = (384, 384, 256)
AG_ORDER = ((2, 1, 0), (1, 0, 2), (0, 2, 1))
RS_ORDER = tuple(tuple(reversed(order)) for order in AG_ORDER)
NEG = -1e30
SEGMENT = 16
N_SEGMENTS = 4
LEAD, TRAIL = 10, 11
AG_STAGES = ((0, (0, 1, 2)), (1, (0, 1, 2)), (2, (0, 1)), (2, (3, 4)))
RS_STAGES = ((0, (3, 4)), (0, (0, 1)), (1, (0, 1, 2)), (2, (0, 1, 2)))
N_STAGES = 4


RS_AT = (0, 5, 11, 16, 20)
AG_AT = (-20, -17, -12, -6, 0)


def columns(half, part):
    order = [(i + half) % 3 for i in range(3)]
    lo = sum(WIDTHS[order[i]] for i in range(part))
    return lo, WIDTHS[order[part]]


def step_table():
    table = {}
    for half in range(2):
        for stage, at in enumerate(RS_AT):
            at += 24 + 8 * half
            table.setdefault(at % 32, []).append(("rs", half, stage, at // 32))
    for half in range(2):
        for stage, at in enumerate(AG_AT):
            at += 8 * half
            table.setdefault(at % 32, []).append(("ag", half, stage, at // 32))
    return table


def kernel(
    x_ref, len_ref, row_ref, column_ref, gamma_ref, w_in_ref, w_kv_ref, w_out_ref, y_ref,
    win, wkv, wout, gfull, hbuf, zbuf, xcur,
    ra, rb0, rb1, rb2,
    k_t, v_ext, q_ext, s_buf, p_buf, mixed,
    ag_send, ag_recv, rs_send, rs_recv, w_local, w_send, w_recv, g_local, g_send, g_recv,
):
    m = lax.axis_index("model")
    core = lax.axis_index("data")
    other = 1 - core
    pos = (lax.div(m, 16), lax.rem(lax.div(m, 4), 4), lax.rem(m, 4))
    rb = (rb0, rb1, rb2)

    def shift(axis, delta):
        return lax.rem(pos[axis] + delta + SIDE, SIDE)

    def neighbour(axis, delta):
        return {"model": m + (shift(axis, delta) - pos[axis]) * STRIDE[axis]}

    barrier = pltpu.get_barrier_semaphore()
    for axis in range(3):
        for delta in (1, -1, 2):
            pl.semaphore_signal(barrier, inc=1, device_id=neighbour(axis, delta), device_id_type=MESH)
    pl.semaphore_signal(barrier, inc=1, device_id={"data": other}, device_id_type=MESH)
    pl.semaphore_wait(barrier, 10)

    pairs = ((w_in_ref, win), (w_kv_ref, wkv), (w_out_ref, wout))

    def weight_local(layer, i):
        src, dst = pairs[i]
        return pltpu.make_async_copy(src.at[layer], dst.at[layer, core], w_local.at[layer, i])

    def weight_send(layer, i):
        src, dst = pairs[i]
        return pltpu.make_async_remote_copy(
            src_ref=src.at[layer], dst_ref=dst.at[layer, core], send_sem=w_send.at[layer, i],
            recv_sem=w_recv.at[layer, i], device_id={"data": other}, device_id_type=MESH)

    def weight_arrival(layer, i):
        src, dst = pairs[i]
        return pltpu.make_async_remote_copy(
            src_ref=src.at[layer], dst_ref=dst.at[layer, other], send_sem=w_send.at[layer, i],
            recv_sem=w_recv.at[layer, i], device_id={"data": other}, device_id_type=MESH)

    def weights_start(layer):
        for i in range(3):
            weight_send(layer, i).start()
            weight_local(layer, i).start()

    def weights_wait(layer):
        for i in range(3):
            weight_local(layer, i).wait()
            weight_send(layer, i).wait_send()
            weight_arrival(layer, i).wait_recv()

    gain_local = pltpu.make_async_copy(gamma_ref, gfull.at[core], g_local)
    gain_send = pltpu.make_async_remote_copy(
        src_ref=gamma_ref, dst_ref=gfull.at[core], send_sem=g_send, recv_sem=g_recv,
        device_id={"data": other}, device_id_type=MESH)
    gain_arrival = pltpu.make_async_remote_copy(
        src_ref=gamma_ref, dst_ref=gfull.at[other], send_sem=g_send, recv_sem=g_recv,
        device_id={"data": other}, device_id_type=MESH)
    gain_send.start()
    gain_local.start()
    weights_start(0)

    def split(where, lo, width, free, piece):
        where = list(where)
        if piece is not None:
            where[free[0]] = pl.ds(2 * piece, 2)
        return where, lo, width

    def h_block(b, half, part, phase, index, piece):
        order = AG_ORDER[part]
        where = [slice(None)] * 3
        for axis in order[phase + 1:]:
            where[axis] = pos[axis]
        where[order[phase]] = index
        where, lo, width = split(where, *columns(half, part), sorted(order[:phase]), piece)
        return hbuf.at[(b, half, *where, slice(None), pl.ds(lo, width))]

    def ag_copy(b, half, part, phase, slot, index, piece, delta):
        block = h_block(b, half, part, phase, index, piece)
        return pltpu.make_async_remote_copy(
            src_ref=block, dst_ref=block, send_sem=ag_send.at[2 * b + half, part, phase, slot],
            recv_sem=ag_recv.at[2 * b + half, part, phase, slot],
            device_id=neighbour(AG_ORDER[part][phase], delta), device_id_type=MESH)

    def ag_sent(b, half, part, phase, slot):
        axis = AG_ORDER[part][phase]
        index, piece, delta = ((pos[axis], None, 1), (pos[axis], None, -1), (pos[axis], None, 2),
                               (shift(axis, -1), 0, 1), (shift(axis, 1), 1, -1))[slot]
        return ag_copy(b, half, part, phase, slot, index, piece, delta)

    def ag_arrival(b, half, part, phase, slot):
        axis = AG_ORDER[part][phase]
        index, piece, delta = ((shift(axis, -1), None, 1), (shift(axis, 1), None, -1), (shift(axis, 2), None, 2),
                               (shift(axis, 2), 0, 1), (shift(axis, 2), 1, -1))[slot]
        return ag_copy(b, half, part, phase, slot, index, piece, delta)

    def ag_step(b, half, stage):
        for part in range(3):
            if stage:
                before, slots = AG_STAGES[stage - 1]
                for slot in slots:
                    ag_arrival(b, half, part, before, slot).wait_recv()
            if stage < N_STAGES:
                phase, slots = AG_STAGES[stage]
                for slot in slots:
                    ag_sent(b, half, part, phase, slot).start()
        if stage == N_STAGES:
            for part in range(3):
                for phase, slots in AG_STAGES:
                    for slot in slots:
                        ag_sent(b, half, part, phase, slot).wait_send()

    def z_where(part, phase, index):
        order = RS_ORDER[part]
        where = [slice(None)] * 3
        for axis in order[:phase]:
            where[axis] = pos[axis]
        where[order[phase]] = index
        return where, sorted(order[phase + 1:])

    def z_block(b, half, part, phase, index, piece):
        where, free = z_where(part, phase, index)
        where, lo, width = split(where, *columns(half, part), free, piece)
        return zbuf.at[(b, half, *where, slice(None), pl.ds(lo, width))]

    def rs_copy(b, half, part, phase, slot):
        axis = RS_ORDER[part][phase]
        piece = slot - 3 if slot >= 3 else None
        where, lo, width = split([slice(None)] * (2 - phase), *columns(half, part), list(range(2 - phase)), piece)
        cells = (*where, slice(None), pl.ds(lo, width))
        if slot >= 3:
            index, delta = shift(axis, 2), (-1, 1)[piece]
            dst = ra.at[(2 * b + half, *cells)]
        else:
            delta = (1, -1, 2)[slot]
            index = shift(axis, delta)
            dst = rb[phase].at[(2 * b + half, slot, *cells)]
        return pltpu.make_async_remote_copy(
            src_ref=z_block(b, half, part, phase, index, piece), dst_ref=dst,
            send_sem=rs_send.at[2 * b + half, part, phase, slot], recv_sem=rs_recv.at[2 * b + half, part, phase, slot],
            device_id=neighbour(axis, delta), device_id_type=MESH)

    def add_into(b, half, part, phase, index, piece, slots):
        where, free = z_where(part, phase, index)
        where, lo, width = split(where, *columns(half, part), free, piece)
        lead = [slice(None)] * len(free)
        if piece is not None:
            lead[0] = where[free[0]]
        target = (b, half, *where, slice(None), pl.ds(lo, width))
        cells = (*lead, slice(None), pl.ds(lo, width))
        total = zbuf[target].astype(F32)
        if piece is not None:
            total = total + ra[(2 * b + half, *cells)].astype(F32)
        for slot in slots:
            total = total + rb[phase][(2 * b + half, slot, *cells)].astype(F32)
        zbuf[target] = total.astype(BF16)

    def rs_step(b, half, stage):
        for part in range(3):
            if stage:
                before, slots = RS_STAGES[stage - 1]
                axis = RS_ORDER[part][before]
                for slot in slots:
                    rs_copy(b, half, part, before, slot).wait_recv()
                if stage == 1:
                    add_into(b, half, part, before, shift(axis, -1), 0, ())
                    add_into(b, half, part, before, shift(axis, 1), 1, ())
                else:
                    add_into(b, half, part, before, pos[axis], None, slots)
            if stage < N_STAGES:
                phase, slots = RS_STAGES[stage]
                for slot in slots:
                    rs_copy(b, half, part, phase, slot).start()
        if stage == N_STAGES:
            for part in range(3):
                for phase, slots in RS_STAGES:
                    for slot in slots:
                        rs_copy(b, half, part, phase, slot).wait_send()

    def norm(b, half, layer):
        x = xcur[b, half].astype(F32)
        gain = jnp.concatenate([gfull[0, layer:layer + 1, :], gfull[1, layer:layer + 1, :]], axis=1).astype(F32)
        inv = lax.rsqrt(jnp.mean(x * x, axis=-1, keepdims=True) + EPSILON)
        hbuf[b, half, pos[0], pos[1], pos[2]] = (x * inv * gain).astype(BF16)

    def residual(b, half):
        z = zbuf[b, half, pos[0], pos[1], pos[2]].astype(F32)
        xcur[b, half] = (xcur[b, half].astype(F32) + z).astype(BF16)

    for half in range(2):
        xcur[:, half] = x_ref[:, half * HALF:(half + 1) * HALF, :]
    gain_local.wait()
    gain_send.wait_send()
    gain_arrival.wait_recv()
    rows_i = lax.broadcasted_iota(jnp.int32, (HEAD, TILE), 0)
    q_ext[:, HEAD:] = jnp.where(lax.broadcasted_iota(jnp.int32, (2 * TILE, HEAD), 1) == 0, 1.0, 0.0).astype(BF16)
    v_ext[:, :, :, HEAD:] = jnp.ones((N_TILES, 2, TILE, HEAD), BF16)

    table = step_table()

    def run(kind, half, stage, seg):
        b = lax.rem(seg, 2)
        if kind == "rs":
            rs_step(b, half, stage)
            if stage == N_STAGES:
                residual(b, half)
        else:
            if stage == 0:
                @pl.when(seg < 2)
                def _():
                    norm(b, half, 0)

                @pl.when(seg >= 2)
                def _():
                    norm(b, half, 1)

            ag_step(b, half, stage)

    def tick(unit, point, lo=0, hi=SEGMENT):
        if not any(phase % 2 == point and lo <= phase // 2 < hi for phase in table):
            return
        place = lax.rem(unit, SEGMENT)
        if hi - lo == 1:
            for kind, half, stage, late in table[2 * lo + point]:
                seg = lax.div(unit, SEGMENT) - 2 - late

                @pl.when(jnp.logical_and(seg >= 0, seg < N_SEGMENTS))
                def _():
                    run(kind, half, stage, seg)
            return
        mid = (lo + hi) // 2

        @pl.when(place < mid)
        def _():
            tick(unit, point, lo, mid)

        @pl.when(place >= mid)
        def _():
            tick(unit, point, mid, hi)

    scale = float(HEAD ** -0.5 * 1.4426950408889634)

    def scores(head, t, half):
        rows = pl.ds(head * TILE, TILE)
        q = q_ext[rows, :]
        q_pos = column_ref[...] + half * HALF
        top = None
        for j in range(t + 1):
            for part in range(2):
                s = jnp.dot(q, k_t[j, part], preferred_element_type=F32)
                if j == t:
                    s = jnp.where(row_ref[...] + part * HALF <= q_pos, s, NEG)
                s_buf[rows, (2 * j + part) * TILE:(2 * j + part + 1) * TILE] = s
                high = jnp.maximum(s[:, :HEAD], s[:, HEAD:])
                top = high if top is None else jnp.maximum(top, high)
        return jnp.max(top, axis=-1, keepdims=True)

    def weigh(head, t, half, top):
        rows = pl.ds(head * TILE, TILE)
        n = 2 * (t + 1)
        for k in range(n):
            cells = (rows, pl.ds(k * TILE, TILE))
            p_buf[cells] = jnp.exp2((s_buf[cells] - top) * scale).astype(BF16)
        out = jnp.dot(
            p_buf[rows, :n * TILE], v_ext[:t + 1].reshape(n * TILE, 2 * HEAD), preferred_element_type=F32)
        mixed[half, t, :, head * HEAD:(head + 1) * HEAD] = (out[:, :HEAD] / out[:, HEAD:]).astype(BF16)

    def attend(t, half):
        tops = [scores(head, t, half) for head in range(2)]
        for head in range(2):
            weigh(head, t, half, tops[head])

    first = 2 * SEGMENT

    @pl.loop(first - LEAD, first + N_SEGMENTS * SEGMENT + TRAIL)
    def _(unit):
        seg = lax.div(unit, SEGMENT) - 2
        layer, b = lax.div(seg, 2), lax.rem(seg, 2)
        half, t = lax.rem(lax.div(unit, 4), 2), lax.rem(unit, 4)
        busy = jnp.logical_and(unit >= first, unit < first + N_SEGMENTS * SEGMENT)
        project = jnp.logical_and(busy, lax.rem(unit, SEGMENT) < 8)
        attention = jnp.logical_and(busy, lax.rem(unit, SEGMENT) >= 8)
        tick(unit, 0)

        @pl.when(unit == first)
        def _():
            weights_wait(0)
            weights_start(1)

        @pl.when(unit == first + 2 * SEGMENT)
        def _():
            weights_wait(1)

        def mlp(i):
            h = hbuf[b, half, t].reshape(TILE, D_MODEL)
            lo = ATTN + i * 512
            g = jnp.dot(h, win[layer, :, :, lo:lo + 512].reshape(D_MODEL, 512), preferred_element_type=F32)
            u = jnp.dot(h, win[layer, :, :, lo + FF:lo + FF + 512].reshape(D_MODEL, 512), preferred_element_type=F32)
            g = g.astype(BF16).astype(F32)
            u = u.astype(BF16).astype(F32)
            mixed[half, t, :, lo:lo + 512] = (jax.nn.silu(g) * u).astype(BF16)

        @pl.when(project)
        def _():
            h = hbuf[b, half, t].reshape(TILE, D_MODEL)
            kv = jnp.dot(h, wkv[layer].reshape(D_MODEL, 2 * HEAD), preferred_element_type=F32).astype(BF16)
            k_t[t, half, :HEAD, :] = kv[:, :HEAD].T
            key_pos = t * (2 * TILE) + half * HALF + row_ref[...]
            hidden = jnp.logical_and(rows_i == 0, key_pos >= len_ref[pl.ds(b, 1), :])
            k_t[t, half, HEAD:, :] = jnp.where(hidden, NEG, 0.0).astype(BF16)
            v_ext[t, half, :, :HEAD] = kv[:, HEAD:]
            mlp(0)

        @pl.when(attention)
        def _():
            h = hbuf[b, half, t].reshape(TILE, D_MODEL)
            q = jnp.dot(h, win[layer, :, :, :ATTN].reshape(D_MODEL, ATTN), preferred_element_type=F32).astype(BF16)
            q_ext[:TILE, :HEAD] = q[:, :HEAD]
            q_ext[TILE:, :HEAD] = q[:, HEAD:]
            for plane in range(N_TILES):
                @pl.when(t == plane)
                def _(plane=plane):
                    attend(plane, half)

        tick(unit, 1)

        @pl.when(project)
        def _():
            mlp(1)

        @pl.when(attention)
        def _():
            for side in range(2):
                z = jnp.dot(mixed[half, t], wout[layer, side], preferred_element_type=F32).astype(BF16)
                zbuf[b, half, t, :, :, :, side * 512:(side + 1) * 512] = z.reshape(SIDE, SIDE, HALF, 512)

    for half in range(2):
        y_ref[:, half * HALF:(half + 1) * HALF, :] = xcur[:, half]


def local_step(x, lengths, gamma, w_in, w_kv, w_out):
    vmem = pl.BlockSpec(memory_space=pltpu.VMEM)
    hbm = pl.BlockSpec(memory_space=pl.ANY)
    dma = pltpu.SemaphoreType.DMA
    box = (SIDE, SIDE)
    scratch = [
        pltpu.VMEM((2, 2, 512, 2304), BF16),
        pltpu.VMEM((2, 2, 512, 256), BF16),
        pltpu.VMEM((2, 2, 1280, 512), BF16),
        pltpu.VMEM((2, 2, 512), BF16),
        pltpu.VMEM((2, 2, SIDE, *box, HALF, D_MODEL), BF16),
        pltpu.VMEM((2, 2, SIDE, *box, HALF, D_MODEL), BF16),
        pltpu.VMEM((2, 2, HALF, D_MODEL), BF16),
        pltpu.VMEM((4, *box, HALF, D_MODEL), BF16),
        pltpu.VMEM((4, 2, *box, HALF, D_MODEL), BF16),
        pltpu.VMEM((4, 3, SIDE, HALF, D_MODEL), BF16),
        pltpu.VMEM((4, 3, HALF, D_MODEL), BF16),
        pltpu.VMEM((N_TILES, 2, 2 * HEAD, TILE), BF16),
        pltpu.VMEM((N_TILES, 2, TILE, 2 * HEAD), BF16),
        pltpu.VMEM((2 * TILE, 2 * HEAD), BF16),
        pltpu.VMEM((2 * TILE, 2 * N_TILES * TILE), F32),
        pltpu.VMEM((2 * TILE, 2 * N_TILES * TILE), BF16),
        pltpu.VMEM((2, N_TILES, TILE, ATTN + FF), BF16),
        dma((4, 3, 3, 5)), dma((4, 3, 3, 5)), dma((4, 3, 3, 5)), dma((4, 3, 3, 5)),
        dma((2, 3)), dma((2, 3)), dma((2, 3)), dma, dma, dma,
    ]
    place = jnp.asarray([i + HALF * (i // HALF) for i in range(TILE)], jnp.int32)
    return pl.pallas_call(
        kernel,
        out_shape=jax.ShapeDtypeStruct(x.shape, x.dtype),
        in_specs=[vmem] * 5 + [hbm] * 3,
        out_specs=vmem,
        scratch_shapes=scratch,
        compiler_params=pltpu.CompilerParams(
            collective_id=0, has_side_effects=True, vmem_limit_bytes=67_043_328),
        name="layers",
    )(x, lengths.reshape(2, 1), place[None], place[:, None], gamma, w_in, w_kv, w_out)


def solution(mesh):
    batch_axes = ("rep", "data")
    in_specs = (
        P(batch_axes, "model", None),
        P(batch_axes),
        P(None, "data"),
        P(None, "data", "model"),
        P(None, "data", None),
        P(None, "model", "data"),
    )
    return jax.shard_map(local_step, mesh=mesh, in_specs=in_specs, out_specs=P(batch_axes, "model", None), check_vma=False)
```

```python
import functools

import jax
import jax.numpy as jnp
from jax import lax
from jax.experimental import pallas as pl
from jax.experimental.pallas import tpu as pltpu
from jax.sharding import PartitionSpec as P

EPSILON = 1e-6
MESH = pl.DeviceIdType.MESH
F32 = jnp.float32
BF16 = jnp.bfloat16

SIDE = 4
ROWS = 32
HALF = 16
D_MODEL = 1024
HEAD = 128
ATTN = 256
FF = 1024
TILE = SIDE * SIDE * HALF
N_TILES = SIDE
STRIDE = (16, 4, 1)
AG_ORDER = ((2, 1, 0), (1, 0, 2), (0, 2, 1))
RS_ORDER = tuple(tuple(reversed(order)) for order in AG_ORDER)
NEG = -1e30
SEGMENT = 16
N_SEGMENTS = 4
LEAD, TRAIL = 12, 12
AG_SENDS = ((0, (0, 1, 2)), (1, (0, 1, 2)), (2, (5, 7, 6, 8)), (2, (3, 4)))
AG_WAITS = ((0, (0, 1, 2)), (1, (0, 1, 2)), (2, (5, 7)), (2, (6, 8, 3, 4)))
RS_SENDS = ((0, (3, 4, 5, 6)), (0, (7, 8)), (1, (0, 1, 2)), (2, (0, 1, 2)))
RS_WAITS = ((0, (3, 4)), (0, (5, 6, 7, 8)), (1, (0, 1, 2)), (2, (0, 1, 2)))
N_STAGES = 4


RS_AT = (0, 5, 10, 15, 20)
AG_AT = (-20, -16, -11, -6, 0)


def columns(kind, half, part):
    widths = [384] * 3
    widths[{"ag": (2, 1), "rs": (0, 2)}[kind][half]] = 256
    return sum(widths[:part]), widths[part]


def step_table():
    table = {}
    for half in range(2):
        for stage, at in enumerate(RS_AT):
            at += 24 + 8 * half
            table.setdefault(at % 32, []).append(("rs", half, stage, at // 32))
    for half in range(2):
        for stage, at in enumerate(AG_AT):
            at += 8 * half
            table.setdefault(at % 32, []).append(("ag", half, stage, at // 32))
    return table


def kernel(
    x_ref, len_ref, row_ref, column_ref, gamma_ref, w_in_ref, w_kv_ref, w_out_ref, y_ref,
    win, wkv, wout, gfull, hbuf, zbuf, xcur,
    ra, rb0, rb1, rb2,
    k_t, v_ext, q_ext, s_buf, p_buf, mixed,
    ag_send, ag_recv, rs_send, rs_recv, w_local, w_send, w_recv, g_local, g_send, g_recv,
):
    m = lax.axis_index("model")
    core = lax.axis_index("data")
    other = 1 - core
    pos = (lax.div(m, 16), lax.rem(lax.div(m, 4), 4), lax.rem(m, 4))
    rb = (rb0, rb1, rb2)

    def shift(axis, delta):
        return lax.rem(pos[axis] + delta + SIDE, SIDE)

    def neighbour(axis, delta):
        return {"model": m + (shift(axis, delta) - pos[axis]) * STRIDE[axis]}

    barrier = pltpu.get_barrier_semaphore()
    for axis in range(3):
        for delta in (1, -1, 2):
            pl.semaphore_signal(barrier, inc=1, device_id=neighbour(axis, delta), device_id_type=MESH)
    pl.semaphore_signal(barrier, inc=1, device_id={"data": other}, device_id_type=MESH)
    pl.semaphore_wait(barrier, 10)

    pairs = ((w_in_ref, win), (w_kv_ref, wkv), (w_out_ref, wout))

    def weight_local(layer, i):
        src, dst = pairs[i]
        return pltpu.make_async_copy(src.at[layer], dst.at[layer, core], w_local.at[layer, i])

    def weight_send(layer, i):
        src, dst = pairs[i]
        return pltpu.make_async_remote_copy(
            src_ref=src.at[layer], dst_ref=dst.at[layer, core], send_sem=w_send.at[layer, i],
            recv_sem=w_recv.at[layer, i], device_id={"data": other}, device_id_type=MESH)

    def weight_arrival(layer, i):
        src, dst = pairs[i]
        return pltpu.make_async_remote_copy(
            src_ref=src.at[layer], dst_ref=dst.at[layer, other], send_sem=w_send.at[layer, i],
            recv_sem=w_recv.at[layer, i], device_id={"data": other}, device_id_type=MESH)

    def weights_start(layer):
        for i in range(3):
            weight_send(layer, i).start()
            weight_local(layer, i).start()

    def weights_wait(layer):
        for i in range(3):
            weight_local(layer, i).wait()
            weight_send(layer, i).wait_send()
            weight_arrival(layer, i).wait_recv()

    gain_local = pltpu.make_async_copy(gamma_ref, gfull.at[core], g_local)
    gain_send = pltpu.make_async_remote_copy(
        src_ref=gamma_ref, dst_ref=gfull.at[core], send_sem=g_send, recv_sem=g_recv,
        device_id={"data": other}, device_id_type=MESH)
    gain_arrival = pltpu.make_async_remote_copy(
        src_ref=gamma_ref, dst_ref=gfull.at[other], send_sem=g_send, recv_sem=g_recv,
        device_id={"data": other}, device_id_type=MESH)
    gain_send.start()
    gain_local.start()
    weights_start(0)

    def split(where, lo, width, free, piece):
        where = list(where)
        if piece is not None:
            where[free[0]] = pl.ds(2 * piece, 2)
        return where, lo, width

    def h_block(b, half, part, phase, index, piece):
        order = AG_ORDER[part]
        where = [slice(None)] * 3
        for axis in order[phase + 1:]:
            where[axis] = pos[axis]
        where[order[phase]] = index
        where, lo, width = split(where, *columns("ag", half, part), sorted(order[:phase]), piece)
        return hbuf.at[(b, half, *where, slice(None), pl.ds(lo, width))]

    def ag_copy(b, half, part, phase, slot, index, piece, delta):
        block = h_block(b, half, part, phase, index, piece)
        return pltpu.make_async_remote_copy(
            src_ref=block, dst_ref=block, send_sem=ag_send.at[2 * b + half, part, phase, slot],
            recv_sem=ag_recv.at[2 * b + half, part, phase, slot],
            device_id=neighbour(AG_ORDER[part][phase], delta), device_id_type=MESH)

    def ag_sent(b, half, part, phase, slot):
        axis = AG_ORDER[part][phase]
        index, piece, delta = ((pos[axis], None, 1), (pos[axis], None, -1), (pos[axis], None, 2),
                               (shift(axis, -1), 0, 1), (shift(axis, 1), 1, -1),
                               (pos[axis], 0, 1), (pos[axis], 1, 1), (pos[axis], 1, -1), (pos[axis], 0, -1))[slot]
        return ag_copy(b, half, part, phase, slot, index, piece, delta)

    def ag_arrival(b, half, part, phase, slot):
        axis = AG_ORDER[part][phase]
        index, piece, delta = ((shift(axis, -1), None, 1), (shift(axis, 1), None, -1), (shift(axis, 2), None, 2),
                               (shift(axis, 2), 0, 1), (shift(axis, 2), 1, -1),
                               (shift(axis, -1), 0, 1), (shift(axis, -1), 1, 1),
                               (shift(axis, 1), 1, -1), (shift(axis, 1), 0, -1))[slot]
        return ag_copy(b, half, part, phase, slot, index, piece, delta)

    def ag_step(b, half, stage):
        for part in range(3):
            if stage:
                before, slots = AG_WAITS[stage - 1]
                for slot in slots:
                    ag_arrival(b, half, part, before, slot).wait_recv()
            if stage < N_STAGES:
                phase, slots = AG_SENDS[stage]
                for slot in slots:
                    ag_sent(b, half, part, phase, slot).start()
        if stage == N_STAGES:
            for part in range(3):
                for phase, slots in AG_SENDS:
                    for slot in slots:
                        ag_sent(b, half, part, phase, slot).wait_send()

    def z_where(part, phase, index):
        order = RS_ORDER[part]
        where = [slice(None)] * 3
        for axis in order[:phase]:
            where[axis] = pos[axis]
        where[order[phase]] = index
        return where, sorted(order[phase + 1:])

    def z_block(b, half, part, phase, index, piece):
        where, free = z_where(part, phase, index)
        where, lo, width = split(where, *columns("rs", half, part), free, piece)
        return zbuf.at[(b, half, *where, slice(None), pl.ds(lo, width))]

    def rs_copy(b, half, part, phase, slot):
        axis = RS_ORDER[part][phase]
        ahead, piece, delta = ((1, None, 1), (-1, None, -1), (2, None, 2), (2, 0, -1), (2, 1, 1),
                               (-1, 1, -1), (1, 0, 1), (-1, 0, -1), (1, 1, 1))[slot]
        index = shift(axis, ahead)
        where, lo, width = split([slice(None)] * (2 - phase), *columns("rs", half, part), list(range(2 - phase)), piece)
        cells = (*where, slice(None), pl.ds(lo, width))
        if ahead == 2 and delta != 2:
            dst = ra.at[(2 * b + half, *cells)]
        else:
            dst = rb[phase].at[(2 * b + half, {1: 0, -1: 1, 2: 2}[delta], *cells)]
        return pltpu.make_async_remote_copy(
            src_ref=z_block(b, half, part, phase, index, piece), dst_ref=dst,
            send_sem=rs_send.at[2 * b + half, part, phase, slot], recv_sem=rs_recv.at[2 * b + half, part, phase, slot],
            device_id=neighbour(axis, delta), device_id_type=MESH)

    def add_into(b, half, part, phase, index, piece, slots):
        where, free = z_where(part, phase, index)
        where, lo, width = split(where, *columns("rs", half, part), free, piece)
        lead = [slice(None)] * len(free)
        if piece is not None:
            lead[0] = where[free[0]]
        target = (b, half, *where, slice(None), pl.ds(lo, width))
        cells = (*lead, slice(None), pl.ds(lo, width))
        total = zbuf[target].astype(F32)
        if piece is not None:
            total = total + ra[(2 * b + half, *cells)].astype(F32)
        for slot in slots:
            total = total + rb[phase][(2 * b + half, slot, *cells)].astype(F32)
        zbuf[target] = total.astype(BF16)

    def rs_step(b, half, stage):
        for part in range(3):
            if stage:
                before, slots = RS_WAITS[stage - 1]
                axis = RS_ORDER[part][before]
                for slot in slots:
                    rs_copy(b, half, part, before, slot).wait_recv()
                if slots == (3, 4):
                    add_into(b, half, part, before, shift(axis, -1), 0, ())
                    add_into(b, half, part, before, shift(axis, 1), 1, ())
                else:
                    add_into(b, half, part, before, pos[axis], None, slots if before else (0, 1))
            if stage < N_STAGES:
                phase, slots = RS_SENDS[stage]
                for slot in slots:
                    rs_copy(b, half, part, phase, slot).start()
        if stage == N_STAGES:
            for part in range(3):
                for phase, slots in RS_SENDS:
                    for slot in slots:
                        rs_copy(b, half, part, phase, slot).wait_send()

    def norm(b, half, layer):
        x = xcur[b, half].astype(F32)
        gain = jnp.concatenate([gfull[0, layer:layer + 1, :], gfull[1, layer:layer + 1, :]], axis=1).astype(F32)
        inv = lax.rsqrt(jnp.mean(x * x, axis=-1, keepdims=True) + EPSILON)
        hbuf[b, half, pos[0], pos[1], pos[2]] = (x * inv * gain).astype(BF16)

    def residual(b, half):
        z = zbuf[b, half, pos[0], pos[1], pos[2]].astype(F32)
        xcur[b, half] = (xcur[b, half].astype(F32) + z).astype(BF16)

    for half in range(2):
        xcur[:, half] = x_ref[:, half * HALF:(half + 1) * HALF, :]
    gain_local.wait()
    gain_send.wait_send()
    gain_arrival.wait_recv()
    rows_i = lax.broadcasted_iota(jnp.int32, (HEAD, TILE), 0)
    ones = jnp.where(lax.broadcasted_iota(jnp.int32, (2 * TILE, HEAD), 1) == 0, 1.0, 0.0).astype(BF16)
    for half in range(2):
        for t in range(N_TILES):
            q_ext[half, t, :, HEAD:] = ones
    v_ext[:, :, :, HEAD:] = jnp.ones((N_TILES, 2, TILE, HEAD), BF16)

    table = step_table()

    def run(kind, half, stage, seg):
        b = lax.rem(seg, 2)
        if kind == "rs":
            rs_step(b, half, stage)
            if stage == N_STAGES:
                residual(b, half)
        else:
            if stage == 0:
                @pl.when(seg < 2)
                def _():
                    norm(b, half, 0)

                @pl.when(seg >= 2)
                def _():
                    norm(b, half, 1)

            ag_step(b, half, stage)

    def tick(unit, point, lo=0, hi=SEGMENT):
        if not any(phase % 2 == point and lo <= phase // 2 < hi for phase in table):
            return
        place = lax.rem(unit, SEGMENT)
        if hi - lo == 1:
            for kind, half, stage, late in table[2 * lo + point]:
                seg = lax.div(unit, SEGMENT) - 2 - late

                @pl.when(jnp.logical_and(seg >= 0, seg < N_SEGMENTS))
                def _():
                    run(kind, half, stage, seg)
            return
        mid = (lo + hi) // 2

        @pl.when(place < mid)
        def _():
            tick(unit, point, lo, mid)

        @pl.when(place >= mid)
        def _():
            tick(unit, point, mid, hi)

    scale = float(HEAD ** -0.5 * 1.4426950408889634)

    def scores(head, t, half):
        rows = pl.ds(head * TILE, TILE)
        q = q_ext[half, t, rows, :]
        q_pos = column_ref[...] + half * HALF
        top = None
        for j in range(t + 1):
            for part in range(2):
                s = jnp.dot(q, k_t[j, part], preferred_element_type=F32)
                if j == t:
                    s = jnp.where(row_ref[...] + part * HALF <= q_pos, s, NEG)
                s_buf[rows, (2 * j + part) * TILE:(2 * j + part + 1) * TILE] = s
                high = jnp.maximum(s[:, :HEAD], s[:, HEAD:])
                top = high if top is None else jnp.maximum(top, high)
        return jnp.max(top, axis=-1, keepdims=True)

    def weigh(head, t, half, top):
        rows = pl.ds(head * TILE, TILE)
        n = 2 * (t + 1)
        for k in range(n):
            cells = (rows, pl.ds(k * TILE, TILE))
            p_buf[cells] = jnp.exp2((s_buf[cells] - top) * scale).astype(BF16)
        out = jnp.dot(
            p_buf[rows, :n * TILE], v_ext[:t + 1].reshape(n * TILE, 2 * HEAD), preferred_element_type=F32)
        mixed[half, t, :, head * HEAD:(head + 1) * HEAD] = (out[:, :HEAD] / out[:, HEAD:]).astype(BF16)

    def attend(t, half):
        tops = [scores(head, t, half) for head in range(2)]
        for head in range(2):
            weigh(head, t, half, tops[head])

    first = 2 * SEGMENT

    @pl.loop(first - LEAD, first + N_SEGMENTS * SEGMENT + TRAIL)
    def _(unit):
        seg = lax.div(unit, SEGMENT) - 2
        layer, b = lax.div(seg, 2), lax.rem(seg, 2)
        half, t = lax.rem(lax.div(unit, 4), 2), lax.rem(unit, 4)
        busy = jnp.logical_and(unit >= first, unit < first + N_SEGMENTS * SEGMENT)
        project = jnp.logical_and(busy, lax.rem(unit, SEGMENT) < 8)
        attention = jnp.logical_and(busy, lax.rem(unit, SEGMENT) >= 8)
        tick(unit, 0)

        @pl.when(unit == first)
        def _():
            weights_wait(0)
            weights_start(1)

        @pl.when(unit == first + 2 * SEGMENT)
        def _():
            weights_wait(1)

        even = lax.rem(t, 2) == 0
        pair = pl.ds(t - lax.rem(t, 2), 2)

        def normed():
            return hbuf[b, half, pair].reshape(2 * TILE, D_MODEL)

        def mlp(i):
            h = normed()
            lo = ATTN + i * 512
            g = jnp.dot(h, win[layer, :, :, lo:lo + 512].reshape(D_MODEL, 512), preferred_element_type=F32)
            u = jnp.dot(h, win[layer, :, :, lo + FF:lo + FF + 512].reshape(D_MODEL, 512), preferred_element_type=F32)
            g = g.astype(BF16).astype(F32)
            u = u.astype(BF16).astype(F32)
            mixed[half, pair, :, lo:lo + 512] = (jax.nn.silu(g) * u).astype(BF16).reshape(2, TILE, 512)

        @pl.when(jnp.logical_and(project, even))
        def _():
            kv = jnp.dot(normed(), wkv[layer].reshape(D_MODEL, 2 * HEAD), preferred_element_type=F32).astype(BF16)
            q = jnp.dot(
                normed(), win[layer, :, :, :ATTN].reshape(D_MODEL, ATTN), preferred_element_type=F32).astype(BF16)
            for k in range(2):
                rows = slice(k * TILE, (k + 1) * TILE)
                k_t[t + k, half, :HEAD, :] = kv[rows, :HEAD].T
                key_pos = (t + k) * (2 * TILE) + half * HALF + row_ref[...]
                hidden = jnp.logical_and(rows_i == 0, key_pos >= len_ref[pl.ds(b, 1), :])
                k_t[t + k, half, HEAD:, :] = jnp.where(hidden, NEG, 0.0).astype(BF16)
                v_ext[t + k, half, :, :HEAD] = kv[rows, HEAD:]
                q_ext[half, t + k, :TILE, :HEAD] = q[rows, :HEAD]
                q_ext[half, t + k, TILE:, :HEAD] = q[rows, HEAD:]

        @pl.when(jnp.logical_and(project, lax.rem(t, 2) == 1))
        def _():
            mlp(1)

        @pl.when(attention)
        def _():
            for plane in range(N_TILES):
                @pl.when(t == plane)
                def _(plane=plane):
                    attend(plane, half)

        tick(unit, 1)

        @pl.when(jnp.logical_and(project, even))
        def _():
            mlp(0)

        @pl.when(jnp.logical_and(attention, lax.rem(t, 2) == 1))
        def _():
            for side in range(2):
                z = jnp.dot(
                    mixed[half, pair].reshape(2 * TILE, ATTN + FF), wout[layer, side], preferred_element_type=F32)
                zbuf[b, half, pair, :, :, :, side * 512:(side + 1) * 512] = z.astype(BF16).reshape(2, SIDE, SIDE, HALF, 512)

    for half in range(2):
        y_ref[:, half * HALF:(half + 1) * HALF, :] = xcur[:, half]


def local_step(x, lengths, gamma, w_in, w_kv, w_out):
    vmem = pl.BlockSpec(memory_space=pltpu.VMEM)
    hbm = pl.BlockSpec(memory_space=pl.ANY)
    dma = pltpu.SemaphoreType.DMA
    box = (SIDE, SIDE)
    scratch = [
        pltpu.VMEM((2, 2, 512, 2304), BF16),
        pltpu.VMEM((2, 2, 512, 256), BF16),
        pltpu.VMEM((2, 2, 1280, 512), BF16),
        pltpu.VMEM((2, 2, 512), BF16),
        pltpu.VMEM((2, 2, SIDE, *box, HALF, D_MODEL), BF16),
        pltpu.VMEM((2, 2, SIDE, *box, HALF, D_MODEL), BF16),
        pltpu.VMEM((2, 2, HALF, D_MODEL), BF16),
        pltpu.VMEM((4, *box, HALF, D_MODEL), BF16),
        pltpu.VMEM((4, 2, *box, HALF, D_MODEL), BF16),
        pltpu.VMEM((4, 3, SIDE, HALF, D_MODEL), BF16),
        pltpu.VMEM((4, 3, HALF, D_MODEL), BF16),
        pltpu.VMEM((N_TILES, 2, 2 * HEAD, TILE), BF16),
        pltpu.VMEM((N_TILES, 2, TILE, 2 * HEAD), BF16),
        pltpu.VMEM((2, N_TILES, 2 * TILE, 2 * HEAD), BF16),
        pltpu.VMEM((2 * TILE, 2 * N_TILES * TILE), F32),
        pltpu.VMEM((2 * TILE, 2 * N_TILES * TILE), BF16),
        pltpu.VMEM((2, N_TILES, TILE, ATTN + FF), BF16),
        dma((4, 3, 3, 9)), dma((4, 3, 3, 9)), dma((4, 3, 3, 9)), dma((4, 3, 3, 9)),
        dma((2, 3)), dma((2, 3)), dma((2, 3)), dma, dma, dma,
    ]
    place = jnp.asarray([i + HALF * (i // HALF) for i in range(TILE)], jnp.int32)
    return pl.pallas_call(
        kernel,
        out_shape=jax.ShapeDtypeStruct(x.shape, x.dtype),
        in_specs=[vmem] * 5 + [hbm] * 3,
        out_specs=vmem,
        scratch_shapes=scratch,
        compiler_params=pltpu.CompilerParams(
            collective_id=0, has_side_effects=True, vmem_limit_bytes=67_043_328),
        name="layers",
    )(x, lengths.reshape(2, 1), place[None], place[:, None], gamma, w_in, w_kv, w_out)


def solution(mesh):
    batch_axes = ("rep", "data")
    in_specs = (
        P(batch_axes, "model", None),
        P(batch_axes),
        P(None, "data"),
        P(None, "data", "model"),
        P(None, "data", None),
        P(None, "model", "data"),
    )
    return jax.shard_map(local_step, mesh=mesh, in_specs=in_specs, out_specs=P(batch_axes, "model", None), check_vma=False)
```

```python
import functools

import jax
import jax.numpy as jnp
from jax import lax
from jax.experimental import pallas as pl
from jax.experimental.pallas import tpu as pltpu
from jax.sharding import PartitionSpec as P

EPSILON = 1e-6
MESH = pl.DeviceIdType.MESH
F32 = jnp.float32
BF16 = jnp.bfloat16

SIDE = 4
ROWS = 32
HALF = 16
D_MODEL = 1024
HEAD = 128
ATTN = 256
FF = 1024
TILE = SIDE * SIDE * HALF
N_TILES = SIDE
STRIDE = (16, 4, 1)
AG_ORDER = ((2, 1, 0), (1, 0, 2), (0, 2, 1))
RS_ORDER = tuple(tuple(reversed(order)) for order in AG_ORDER)
NEG = -1e30
SEGMENT = 16
N_SEGMENTS = 4
LEAD, TRAIL = 10, 11
AG_SENDS = ((0, (0, 1, 2)), (1, (0, 1, 2)), (2, (5, 7, 6, 8)), (2, (3, 4)))
AG_WAITS = ((0, (0, 1, 2)), (1, (0, 1, 2)), (2, (5, 7)), (2, (6, 8, 3, 4)))
RS_SENDS = ((0, (3, 4, 5, 6)), (0, (7, 8)), (1, (0, 1, 2)), (2, (0, 1, 2)))
RS_WAITS = ((0, (3, 4)), (0, (5, 6, 7, 8)), (1, (0, 1, 2)), (2, (0, 1, 2)))
N_STAGES = 4


RS_AT = (0, 5, 10, 15, 20)
AG_AT = (-20, -16, -11, -6, 0)


def columns(kind, half, part):
    widths = [384] * 3
    widths[{"ag": (2, 1), "rs": (0, 2)}[kind][half]] = 256
    return sum(widths[:part]), widths[part]


def step_table():
    table = {}
    for half in range(2):
        for stage, at in enumerate(RS_AT):
            at += 24 + 8 * half
            table.setdefault(at % 32, []).append(("rs", half, stage, at // 32))
    for half in range(2):
        for stage, at in enumerate(AG_AT):
            at += 8 * half
            table.setdefault(at % 32, []).append(("ag", half, stage, at // 32))
    for steps in table.values():
        if steps[0][0] == "rs" and steps[0][2] == 0 and steps[-1][0] == "ag" and steps[-1][2] < N_STAGES:
            steps.reverse()
    return table


def kernel(
    x_ref, len_ref, row_ref, column_ref, gamma_ref, w_in_ref, w_kv_ref, w_out_ref, y_ref,
    win, wkv, wout, gfull, hbuf, zbuf, xcur,
    ra, rb0, rb1, rb2,
    k_t, v_ext, q_ext, s_buf, p_buf, mixed,
    ag_send, ag_recv, rs_send, rs_recv, w_local, w_send, w_recv, g_local, g_send, g_recv,
):
    m = lax.axis_index("model")
    core = lax.axis_index("data")
    other = 1 - core
    pos = (lax.div(m, 16), lax.rem(lax.div(m, 4), 4), lax.rem(m, 4))
    rb = (rb0, rb1, rb2)

    def shift(axis, delta):
        return lax.rem(pos[axis] + delta + SIDE, SIDE)

    def neighbour(axis, delta):
        return {"model": m + (shift(axis, delta) - pos[axis]) * STRIDE[axis]}

    barrier = pltpu.get_barrier_semaphore()
    for axis in range(3):
        for delta in (1, -1, 2):
            pl.semaphore_signal(barrier, inc=1, device_id=neighbour(axis, delta), device_id_type=MESH)
    pl.semaphore_signal(barrier, inc=1, device_id={"data": other}, device_id_type=MESH)
    pl.semaphore_wait(barrier, 10)

    pairs = ((w_in_ref, win), (w_kv_ref, wkv), (w_out_ref, wout))

    def weight_local(layer, i):
        src, dst = pairs[i]
        return pltpu.make_async_copy(src.at[layer], dst.at[layer, core], w_local.at[layer, i])

    def weight_send(layer, i):
        src, dst = pairs[i]
        return pltpu.make_async_remote_copy(
            src_ref=src.at[layer], dst_ref=dst.at[layer, core], send_sem=w_send.at[layer, i],
            recv_sem=w_recv.at[layer, i], device_id={"data": other}, device_id_type=MESH)

    def weight_arrival(layer, i):
        src, dst = pairs[i]
        return pltpu.make_async_remote_copy(
            src_ref=src.at[layer], dst_ref=dst.at[layer, other], send_sem=w_send.at[layer, i],
            recv_sem=w_recv.at[layer, i], device_id={"data": other}, device_id_type=MESH)

    def weights_start(layer):
        for i in range(3):
            weight_send(layer, i).start()
            weight_local(layer, i).start()

    def weights_wait(layer):
        for i in range(3):
            weight_local(layer, i).wait()
            weight_send(layer, i).wait_send()
            weight_arrival(layer, i).wait_recv()

    gain_local = pltpu.make_async_copy(gamma_ref, gfull.at[core], g_local)
    gain_send = pltpu.make_async_remote_copy(
        src_ref=gamma_ref, dst_ref=gfull.at[core], send_sem=g_send, recv_sem=g_recv,
        device_id={"data": other}, device_id_type=MESH)
    gain_arrival = pltpu.make_async_remote_copy(
        src_ref=gamma_ref, dst_ref=gfull.at[other], send_sem=g_send, recv_sem=g_recv,
        device_id={"data": other}, device_id_type=MESH)
    gain_send.start()
    gain_local.start()

    def split(where, lo, width, free, piece):
        where = list(where)
        if piece is not None:
            where[free[0]] = pl.ds(2 * piece, 2)
        return where, lo, width

    def h_block(b, half, part, phase, index, piece):
        order = AG_ORDER[part]
        where = [slice(None)] * 3
        for axis in order[phase + 1:]:
            where[axis] = pos[axis]
        where[order[phase]] = index
        where, lo, width = split(where, *columns("ag", half, part), sorted(order[:phase]), piece)
        return hbuf.at[(b, half, *where, slice(None), pl.ds(lo, width))]

    def ag_copy(b, half, part, phase, slot, index, piece, delta):
        block = h_block(b, half, part, phase, index, piece)
        return pltpu.make_async_remote_copy(
            src_ref=block, dst_ref=block, send_sem=ag_send.at[2 * b + half, part, phase, slot],
            recv_sem=ag_recv.at[2 * b + half, part, phase, slot],
            device_id=neighbour(AG_ORDER[part][phase], delta), device_id_type=MESH)

    def ag_sent(b, half, part, phase, slot):
        axis = AG_ORDER[part][phase]
        index, piece, delta = ((pos[axis], None, 1), (pos[axis], None, -1), (pos[axis], None, 2),
                               (shift(axis, -1), 0, 1), (shift(axis, 1), 1, -1),
                               (pos[axis], 0, 1), (pos[axis], 1, 1), (pos[axis], 1, -1), (pos[axis], 0, -1))[slot]
        return ag_copy(b, half, part, phase, slot, index, piece, delta)

    def ag_arrival(b, half, part, phase, slot):
        axis = AG_ORDER[part][phase]
        index, piece, delta = ((shift(axis, -1), None, 1), (shift(axis, 1), None, -1), (shift(axis, 2), None, 2),
                               (shift(axis, 2), 0, 1), (shift(axis, 2), 1, -1),
                               (shift(axis, -1), 0, 1), (shift(axis, -1), 1, 1),
                               (shift(axis, 1), 1, -1), (shift(axis, 1), 0, -1))[slot]
        return ag_copy(b, half, part, phase, slot, index, piece, delta)

    def ag_step(b, half, stage):
        for part in range(3):
            if stage:
                before, slots = AG_WAITS[stage - 1]
                for slot in slots:
                    ag_arrival(b, half, part, before, slot).wait_recv()
            if stage < N_STAGES:
                phase, slots = AG_SENDS[stage]
                for slot in slots:
                    ag_sent(b, half, part, phase, slot).start()
        if stage == N_STAGES:
            for part in range(3):
                for phase, slots in AG_SENDS:
                    for slot in slots:
                        ag_sent(b, half, part, phase, slot).wait_send()

    def z_where(part, phase, index):
        order = RS_ORDER[part]
        where = [slice(None)] * 3
        for axis in order[:phase]:
            where[axis] = pos[axis]
        where[order[phase]] = index
        return where, sorted(order[phase + 1:])

    def z_block(b, half, part, phase, index, piece):
        where, free = z_where(part, phase, index)
        where, lo, width = split(where, *columns("rs", half, part), free, piece)
        return zbuf.at[(b, half, *where, slice(None), pl.ds(lo, width))]

    def rs_copy(b, half, part, phase, slot):
        axis = RS_ORDER[part][phase]
        ahead, piece, delta = ((1, None, 1), (-1, None, -1), (2, None, 2), (2, 0, -1), (2, 1, 1),
                               (-1, 1, -1), (1, 0, 1), (-1, 0, -1), (1, 1, 1))[slot]
        index = shift(axis, ahead)
        where, lo, width = split([slice(None)] * (2 - phase), *columns("rs", half, part), list(range(2 - phase)), piece)
        cells = (*where, slice(None), pl.ds(lo, width))
        if ahead == 2 and delta != 2:
            dst = ra.at[(2 * b + half, *cells)]
        else:
            dst = rb[phase].at[(2 * b + half, {1: 0, -1: 1, 2: 2}[delta], *cells)]
        return pltpu.make_async_remote_copy(
            src_ref=z_block(b, half, part, phase, index, piece), dst_ref=dst,
            send_sem=rs_send.at[2 * b + half, part, phase, slot], recv_sem=rs_recv.at[2 * b + half, part, phase, slot],
            device_id=neighbour(axis, delta), device_id_type=MESH)

    def add_into(b, half, part, phase, index, piece, slots):
        where, free = z_where(part, phase, index)
        where, lo, width = split(where, *columns("rs", half, part), free, piece)
        lead = [slice(None)] * len(free)
        if piece is not None:
            lead[0] = where[free[0]]
        target = (b, half, *where, slice(None), pl.ds(lo, width))
        cells = (*lead, slice(None), pl.ds(lo, width))
        total = zbuf[target].astype(F32)
        if piece is not None:
            total = total + ra[(2 * b + half, *cells)].astype(F32)
        for slot in slots:
            total = total + rb[phase][(2 * b + half, slot, *cells)].astype(F32)
        zbuf[target] = total.astype(BF16)

    def rs_step(b, half, stage):
        for part in range(3):
            if stage:
                before, slots = RS_WAITS[stage - 1]
                axis = RS_ORDER[part][before]
                for slot in slots:
                    rs_copy(b, half, part, before, slot).wait_recv()
                if slots == (3, 4):
                    add_into(b, half, part, before, shift(axis, -1), 0, ())
                    add_into(b, half, part, before, shift(axis, 1), 1, ())
                else:
                    add_into(b, half, part, before, pos[axis], None, slots if before else (0, 1))
            if stage < N_STAGES:
                phase, slots = RS_SENDS[stage]
                for slot in slots:
                    rs_copy(b, half, part, phase, slot).start()
        if stage == N_STAGES:
            for part in range(3):
                for phase, slots in RS_SENDS:
                    for slot in slots:
                        rs_copy(b, half, part, phase, slot).wait_send()

    def norm(b, half, layer):
        x = xcur[b, half].astype(F32)
        gain = jnp.concatenate([gfull[0, layer:layer + 1, :], gfull[1, layer:layer + 1, :]], axis=1).astype(F32)
        inv = lax.rsqrt(jnp.mean(x * x, axis=-1, keepdims=True) + EPSILON)
        hbuf[b, half, pos[0], pos[1], pos[2]] = (x * inv * gain).astype(BF16)

    def residual(b, half):
        z = zbuf[b, half, pos[0], pos[1], pos[2]].astype(F32)
        xcur[b, half] = (xcur[b, half].astype(F32) + z).astype(BF16)

    for half in range(2):
        xcur[:, half] = x_ref[:, half * HALF:(half + 1) * HALF, :]
    gain_local.wait()
    gain_send.wait_send()
    gain_arrival.wait_recv()
    rows_i = lax.broadcasted_iota(jnp.int32, (HEAD, TILE), 0)
    ones = jnp.where(lax.broadcasted_iota(jnp.int32, (2 * TILE, HEAD), 1) == 0, 1.0, 0.0).astype(BF16)
    for half in range(2):
        for t in range(N_TILES):
            q_ext[half, t, :, HEAD:] = ones
    v_ext[:, :, :, HEAD:] = jnp.ones((N_TILES, 2, TILE, HEAD), BF16)

    table = step_table()

    def run(kind, half, stage, seg):
        b = lax.rem(seg, 2)
        if kind == "rs":
            rs_step(b, half, stage)
            if stage == N_STAGES:
                residual(b, half)
        else:
            if stage == 0:
                @pl.when(seg < 2)
                def _():
                    norm(b, half, 0)

                @pl.when(seg >= 2)
                def _():
                    norm(b, half, 1)

            ag_step(b, half, stage)

    def tick(unit, point, lo=0, hi=SEGMENT):
        if not any(phase % 2 == point and lo <= phase // 2 < hi for phase in table):
            return
        place = lax.rem(unit, SEGMENT)
        if hi - lo == 1:
            for kind, half, stage, late in table[2 * lo + point]:
                seg = lax.div(unit, SEGMENT) - 2 - late

                @pl.when(jnp.logical_and(seg >= 0, seg < N_SEGMENTS))
                def _():
                    run(kind, half, stage, seg)
            return
        mid = (lo + hi) // 2

        @pl.when(place < mid)
        def _():
            tick(unit, point, lo, mid)

        @pl.when(place >= mid)
        def _():
            tick(unit, point, mid, hi)

    scale = float(HEAD ** -0.5 * 1.4426950408889634)

    def scores(head, t, half):
        rows = pl.ds(head * TILE, TILE)
        q = q_ext[half, t, rows, :]
        q_pos = column_ref[...] + half * HALF
        top = None
        for j in range(t + 1):
            for part in range(2):
                s = jnp.dot(q, k_t[j, part], preferred_element_type=F32)
                if j == t:
                    s = jnp.where(row_ref[...] + part * HALF <= q_pos, s, NEG)
                s_buf[rows, (2 * j + part) * TILE:(2 * j + part + 1) * TILE] = s
                high = jnp.maximum(s[:, :HEAD], s[:, HEAD:])
                top = high if top is None else jnp.maximum(top, high)
        return jnp.max(top, axis=-1, keepdims=True)

    def weigh(head, t, half, top):
        rows = pl.ds(head * TILE, TILE)
        n = 2 * (t + 1)
        for k in range(n):
            cells = (rows, pl.ds(k * TILE, TILE))
            p_buf[cells] = jnp.exp2((s_buf[cells] - top) * scale).astype(BF16)
        out = jnp.dot(
            p_buf[rows, :n * TILE], v_ext[:t + 1].reshape(n * TILE, 2 * HEAD), preferred_element_type=F32)
        mixed[half, t, :, head * HEAD:(head + 1) * HEAD] = (out[:, :HEAD] / out[:, HEAD:]).astype(BF16)

    def attend(t, half):
        tops = [scores(head, t, half) for head in range(2)]
        for head in range(2):
            weigh(head, t, half, tops[head])

    first = 2 * SEGMENT

    @pl.loop(first - LEAD, first + N_SEGMENTS * SEGMENT + TRAIL)
    def _(unit):
        seg = lax.div(unit, SEGMENT) - 2
        layer, b = lax.div(seg, 2), lax.rem(seg, 2)
        half, t = lax.rem(lax.div(unit, 4), 2), lax.rem(unit, 4)
        busy = jnp.logical_and(unit >= first, unit < first + N_SEGMENTS * SEGMENT)
        project = jnp.logical_and(busy, lax.rem(unit, SEGMENT) < 8)
        attention = jnp.logical_and(busy, lax.rem(unit, SEGMENT) >= 8)
        tick(unit, 0)

        @pl.when(unit == first - LEAD)
        def _():
            weights_start(0)

        @pl.when(unit == first)
        def _():
            weights_wait(0)
            weights_start(1)

        @pl.when(unit == first + 2 * SEGMENT)
        def _():
            weights_wait(1)

        even = lax.rem(t, 2) == 0
        pair = pl.ds(t - lax.rem(t, 2), 2)

        def normed():
            return hbuf[b, half, pair].reshape(2 * TILE, D_MODEL)

        def mlp(i):
            h = normed()
            lo = ATTN + i * 512
            g = jnp.dot(h, win[layer, :, :, lo:lo + 512].reshape(D_MODEL, 512), preferred_element_type=F32)
            u = jnp.dot(h, win[layer, :, :, lo + FF:lo + FF + 512].reshape(D_MODEL, 512), preferred_element_type=F32)
            g = g.astype(BF16).astype(F32)
            u = u.astype(BF16).astype(F32)
            mixed[half, pair, :, lo:lo + 512] = (jax.nn.silu(g) * u).astype(BF16).reshape(2, TILE, 512)

        @pl.when(jnp.logical_and(project, even))
        def _():
            kv = jnp.dot(normed(), wkv[layer].reshape(D_MODEL, 2 * HEAD), preferred_element_type=F32).astype(BF16)
            q = jnp.dot(
                normed(), win[layer, :, :, :ATTN].reshape(D_MODEL, ATTN), preferred_element_type=F32).astype(BF16)
            for k in range(2):
                rows = slice(k * TILE, (k + 1) * TILE)
                k_t[t + k, half, :HEAD, :] = kv[rows, :HEAD].T
                key_pos = (t + k) * (2 * TILE) + half * HALF + row_ref[...]
                hidden = jnp.logical_and(rows_i == 0, key_pos >= len_ref[pl.ds(b, 1), :])
                k_t[t + k, half, HEAD:, :] = jnp.where(hidden, NEG, 0.0).astype(BF16)
                v_ext[t + k, half, :, :HEAD] = kv[rows, HEAD:]
                q_ext[half, t + k, :TILE, :HEAD] = q[rows, :HEAD]
                q_ext[half, t + k, TILE:, :HEAD] = q[rows, HEAD:]

        @pl.when(jnp.logical_and(project, lax.rem(t, 2) == 1))
        def _():
            mlp(1)

        @pl.when(attention)
        def _():
            for plane in range(N_TILES):
                @pl.when(t == plane)
                def _(plane=plane):
                    attend(plane, half)

        tick(unit, 1)

        @pl.when(jnp.logical_and(project, even))
        def _():
            mlp(0)

        @pl.when(jnp.logical_and(attention, lax.rem(t, 2) == 1))
        def _():
            for side in range(2):
                z = jnp.dot(
                    mixed[half, pair].reshape(2 * TILE, ATTN + FF), wout[layer, side], preferred_element_type=F32)
                zbuf[b, half, pair, :, :, :, side * 512:(side + 1) * 512] = z.astype(BF16).reshape(2, SIDE, SIDE, HALF, 512)

    for half in range(2):
        y_ref[:, half * HALF:(half + 1) * HALF, :] = xcur[:, half]


def local_step(x, lengths, gamma, w_in, w_kv, w_out):
    vmem = pl.BlockSpec(memory_space=pltpu.VMEM)
    hbm = pl.BlockSpec(memory_space=pl.ANY)
    dma = pltpu.SemaphoreType.DMA
    box = (SIDE, SIDE)
    scratch = [
        pltpu.VMEM((2, 2, 512, 2304), BF16),
        pltpu.VMEM((2, 2, 512, 256), BF16),
        pltpu.VMEM((2, 2, 1280, 512), BF16),
        pltpu.VMEM((2, 2, 512), BF16),
        pltpu.VMEM((2, 2, SIDE, *box, HALF, D_MODEL), BF16),
        pltpu.VMEM((2, 2, SIDE, *box, HALF, D_MODEL), BF16),
        pltpu.VMEM((2, 2, HALF, D_MODEL), BF16),
        pltpu.VMEM((4, *box, HALF, D_MODEL), BF16),
        pltpu.VMEM((4, 2, *box, HALF, D_MODEL), BF16),
        pltpu.VMEM((4, 3, SIDE, HALF, D_MODEL), BF16),
        pltpu.VMEM((4, 3, HALF, D_MODEL), BF16),
        pltpu.VMEM((N_TILES, 2, 2 * HEAD, TILE), BF16),
        pltpu.VMEM((N_TILES, 2, TILE, 2 * HEAD), BF16),
        pltpu.VMEM((2, N_TILES, 2 * TILE, 2 * HEAD), BF16),
        pltpu.VMEM((2 * TILE, 2 * N_TILES * TILE), F32),
        pltpu.VMEM((2 * TILE, 2 * N_TILES * TILE), BF16),
        pltpu.VMEM((2, N_TILES, TILE, ATTN + FF), BF16),
        dma((4, 3, 3, 9)), dma((4, 3, 3, 9)), dma((4, 3, 3, 9)), dma((4, 3, 3, 9)),
        dma((2, 3)), dma((2, 3)), dma((2, 3)), dma, dma, dma,
    ]
    place = jnp.asarray([i + HALF * (i // HALF) for i in range(TILE)], jnp.int32)
    return pl.pallas_call(
        kernel,
        out_shape=jax.ShapeDtypeStruct(x.shape, x.dtype),
        in_specs=[vmem] * 5 + [hbm] * 3,
        out_specs=vmem,
        scratch_shapes=scratch,
        compiler_params=pltpu.CompilerParams(
            collective_id=0, has_side_effects=True, vmem_limit_bytes=67_043_328),
        name="layers",
    )(x, lengths.reshape(2, 1), place[None], place[:, None], gamma, w_in, w_kv, w_out)


def solution(mesh):
    batch_axes = ("rep", "data")
    in_specs = (
        P(batch_axes, "model", None),
        P(batch_axes),
        P(None, "data"),
        P(None, "data", "model"),
        P(None, "data", None),
        P(None, "model", "data"),
    )
    return jax.shard_map(local_step, mesh=mesh, in_specs=in_specs, out_specs=P(batch_axes, "model", None), check_vma=False)
```
